32 devices in a mesh: mkt: 8 (over z, x), grp: 4 (over y, core).
Axes of the slice: x: 2, y: 2, z: 4, core: 2. Of those that a mesh axis runs over, the one named last changes fastest.
Arguments:
- mean_utility: float32 [512, 64], P(('mkt', 'grp')), may hold values from -5 to -1
- market_share: float32 [512, 64], P(('mkt', 'grp')), may hold values from 0.001 to 0.02
- product_traits: float32 [512, 64, 5], P(('mkt', 'grp')), may hold values from -1 to 1
- taste_draws: float32 [512, 5, 1024], P(('mkt', 'grp')), may hold values from -4 to 4
- taste_scale: float32 [5], replicated, may hold values from 0.3 to 1
- type_weight: float32 [512, 1024], P(('mkt', 'grp')), may hold values from 0.1 to 1
- market_size: float32 [512], P(('mkt', 'grp')), may hold values from 0.05 to 3
- product_firm: int32 [512, 64], P(('mkt', 'grp')), may hold values from 0 to 511, all different within a row
- firm_order: int32 [512], replicated, may hold values from 0 to 511, each once
- loyalty: float32 [512, 1024], P(('mkt', 'grp')), may hold values from -1 to 1
- firm_share: float32 [512, 1024], replicated, may hold values from 2e-05 to 0.15
Outputs:
- utility_out: float32 [512, 64], P(('mkt', 'grp'))
- loyalty_out: float32 [512, 1024], P(('mkt', 'grp'))
The draws below stay inside these ranges and needn't reach their ends.
Inputs may be any that keep to these rules, and one draw needn't show every extreme that they name: `product_firm`: in each market the 64 products belong to 64 different firms, and every firm sells in some market. `firm_order`: each firm appears once.
All inputs are finite; a program needn't handle non-finite values.
Results may differ from the reference program's by a relative error of at most 0.0001.
Values sent between devices are 32-bit elements; how exact they have to be, the bound alone decides.
A program may use at most 64 MiB of HBM per device.

```python
import math
import jax
import jax.numpy as jnp
from jax import lax

J = 64
FIRMS = 512
R = 1024
K = 5
ITERS = 3
M_DEV = 16
MARKETS = 512


def draw_market_size(key, part):
    index = jnp.arange(MARKETS, dtype=jnp.float32)
    base = 1.0 + 2.0 * index / max(MARKETS - 1, 1)
    factor = jnp.exp(jax.random.uniform(key, (MARKETS,), jnp.float32, jnp.log(0.05), 0.0))
    return base * factor


def draw_firm_share(key, part):
    key_firm = jax.random.fold_in(key, 11)
    key_type = jax.random.fold_in(key, 12)
    key_noise = jax.random.fold_in(key, 13)
    firm_level = jax.random.uniform(key_firm, (FIRMS, 1), jnp.float32, -2.5, 2.5)
    noise = jnp.clip(0.5 * jax.random.normal(key_noise, (FIRMS, R), jnp.float32), -1.0, 1.0)
    type_level = jax.random.uniform(key_type, (1, R), jnp.float32, -0.5, 0.5)
    return jnp.exp(-6.5 + firm_level + type_level + noise)


def shard_levels(stream_key, shape, cuts, low, high):
    level = 1.0
    for position, shards_of in cuts:
        draws = jax.random.uniform(jax.random.fold_in(jax.random.fold_in(stream_key, 6), position), (shards_of,), jnp.float32, low / len(cuts), high / len(cuts))
        level = level * jnp.repeat(jnp.exp(draws), shape[position] // shards_of).reshape((-1,) + (1,) * (len(shape) - 1 - position))
    return level


def distinct(own_key, rows, number_of, top, lift):
    ranking = jax.random.permutation(jax.random.fold_in(own_key, 1), number_of)
    pull = ranking
    for power in range(3):
        pull = pull * pull // number_of
    pull = pull * lift // number_of
    tickets = jax.random.randint(jax.random.fold_in(own_key, 2), (rows, number_of), 0, 4096) + pull
    fixed_rows = jax.random.permutation(jax.random.fold_in(own_key, 3), rows)[jnp.arange(number_of) % rows]
    tickets = jnp.where(jnp.arange(rows)[:, None] == fixed_rows[None, :], 1 << 14, tickets)
    score = tickets * number_of + jnp.arange(number_of)
    return lax.top_k(score.astype(jnp.int32), top)[1].astype(jnp.int32)


def scatter_about(stream_key, shape, spread, most, split=(), kind=jnp.bfloat16):
    level = shard_levels(stream_key, shape, split, -0.22, 0.18) if split else 1.0
    values = jax.random.normal(stream_key, shape, jnp.float32) * spread * level
    return jnp.minimum(jnp.maximum(values, -most), most).astype(kind)


def setup_inputs(seed: int = 0) -> dict:
    seeds = jax.random.split(jax.random.key(seed), 12)
    return {
        "mean_utility": jnp.clip(-5.0 + 4.0 * jax.random.uniform(seeds[0], (MARKETS, J), jnp.float32) ** shard_levels(seeds[0], (MARKETS, J), ((0, 32),), -0.2, 0.2), -5.0, -1.0),
        "market_share": jnp.clip(jnp.exp(math.log(0.02) - 2.9957322 * jax.random.uniform(seeds[1], (MARKETS, J), jnp.float32) ** shard_levels(seeds[1], (MARKETS, J), ((0, 32),), -0.2, 0.2)), 0.001, 0.02),
        "product_traits": jnp.clip(jax.random.uniform(seeds[2], (MARKETS, J, K), jnp.float32, -1.0, 1.0) * shard_levels(seeds[2], (MARKETS, J, K), ((0, 32),), -0.4, 0.0), -1.0, 1.0),
        "taste_draws": scatter_about(seeds[3], (MARKETS, K, R), 1.0, 4.0, ((0, 32),), jnp.float32),
        "taste_scale": jnp.clip(jnp.exp(jax.random.uniform(seeds[4], (K,), jnp.float32, math.log(0.3), math.log(1.0))), 0.3, 1.0),
        "type_weight": jnp.clip(jnp.exp(math.log(1.0) - 2.3025851 * jax.random.uniform(seeds[5], (MARKETS, R), jnp.float32) ** shard_levels(seeds[5], (MARKETS, R), ((0, 32),), -0.2, 0.2)), 0.1, 1.0),
        "market_size": draw_market_size(jax.random.fold_in(seeds[11], 71), 0),
        "product_firm": distinct(seeds[7], MARKETS, FIRMS, J, 1024),
        "firm_order": jax.random.permutation(seeds[8], FIRMS).astype(jnp.int32),
        "loyalty": jnp.clip(jax.random.uniform(seeds[9], (FIRMS, R), jnp.float32, -1.0, 1.0) * shard_levels(seeds[9], (FIRMS, R), ((0, 32),), -0.4, 0.0), -1.0, 1.0),
        "firm_share": draw_firm_share(jax.random.fold_in(seeds[11], 71), 0),
    }


clip_target = 0.5
norm_eps = 1e-06

def market_terms(mean_block, traits_block, draws_block, weight_block, size_block, firms_block, table, taste_scale):
    taste = jnp.einsum('mjk,mkr->mjr', traits_block * taste_scale, draws_block, precision=lax.Precision.HIGHEST)
    expu = jnp.exp(mean_block[:, :, None] + taste + jnp.take(table, firms_block, axis=0))
    choice_prob = expu / (1.0 + lax.optimization_barrier(jnp.sum(expu, axis=1, keepdims=True)))
    predicted = jnp.einsum('mjr,mr->mj', choice_prob, weight_block, precision=lax.Precision.HIGHEST) / lax.optimization_barrier(jnp.sum(weight_block, axis=1))[:, None]
    weighted = choice_prob * (size_block[:, None] * weight_block)[:, None, :]
    partial_value = jax.ops.segment_sum(weighted.reshape(-1, weighted.shape[2]), firms_block.reshape(-1), num_segments=table.shape[0])
    return (predicted, partial_value)

def reference(mean_utility, market_share, product_traits, taste_draws, taste_scale, type_weight, market_size, product_firm, firm_order, loyalty, firm_share):
    blocks = MARKETS // M_DEV
    table = jnp.zeros((FIRMS, R), loyalty.dtype).at[firm_order].set(loyalty)
    type_mass = lax.optimization_barrier(jnp.sum(market_size[:, None] * type_weight, axis=0))
    traits_b = product_traits.reshape(blocks, M_DEV, J, K)
    draws_b = taste_draws.reshape(blocks, M_DEV, K, R)
    weight_b = type_weight.reshape(blocks, M_DEV, R)
    size_b = market_size.reshape(blocks, M_DEV)
    firms_b = product_firm.reshape(blocks, M_DEV, J)
    mean_now = mean_utility
    for step in range(ITERS):
        mean_b = mean_now.reshape(blocks, M_DEV, J)

        def scan_block(carry, pieces):
            predicted, partial_value = market_terms(pieces[0], pieces[1], pieces[2], pieces[3], pieces[4], pieces[5], table, taste_scale)
            return (carry + partial_value, predicted)
        totals, predicted = lax.scan(scan_block, jnp.zeros((FIRMS, R), jnp.float32), (mean_b, traits_b, draws_b, weight_b, size_b, firms_b))
        gap = jnp.log(firm_share) - jnp.log(totals / type_mass[None, :])
        clip = jnp.minimum(1.0, clip_target / jnp.sqrt(jnp.mean(gap * gap) + norm_eps))
        table = table + clip * gap
        mean_now = mean_now + jnp.log(market_share) - jnp.log(predicted.reshape(MARKETS, J))
    return (mean_now, jnp.take(table, firm_order, axis=0))
```

```python
import functools
import math

import jax
import jax.numpy as jnp
from jax import lax
from jax.experimental import pallas as pl
from jax.experimental.pallas import tpu as pltpu
from jax.sharding import PartitionSpec as P

ITERS = 3
LANES = 128
MESH = pl.DeviceIdType.MESH

clip_target = 0.5
norm_eps = 1e-06


def columns(row):
    return jnp.broadcast_to(row, (LANES, LANES)).T


def split_hi_lo(x):
    hi = x.astype(jnp.bfloat16)
    lo = (x - hi.astype(jnp.float32)).astype(jnp.bfloat16)
    return hi, lo


def kernel(
    dims,
    wide_ref, info_ref, loy_ref, base_ref, mean0_ref, order_ref, share_ref,
    mean_out, loy_out,
    wide, info, loy, means, tbl, tq, tmass, tm_own,
    one_hot, one_hot_t, taste, order_col, share_v, weighted, table_hl, acc,
    sums, sums_in, totals, totals_in, gap, squares, squares_in, old, old_in, last, last_in,
    copy_sem, wide_s, info_s, loy_s, mean_s, tq_s, tm_s, sums_s, totals_s, gap_s, old_s, last_s, sq_s,
):
    mkt, grp, rb, groups, n_m, J, K, firms, owned, R = dims
    n = mkt * grp
    rows = n_m * J
    tiles = rows // LANES
    qr = firms // groups
    a = lax.axis_index("mkt")
    b = lax.axis_index("grp")
    ao, ai = a // rb, a % rb
    q_me = ao * grp + b
    me = a * grp + b

    def type_peer(d):
        p = (ai + d) % rb
        return p, (ao * rb + p, b)

    def market_peer(d):
        q = (q_me + d) % groups
        return q, ((q // grp) * rb + ai, q % grp)

    pending = []

    def send(src, dst, sems, mine, theirs, device):
        copy = pltpu.make_async_remote_copy(
            src_ref=src, dst_ref=dst.at[mine], send_sem=sems.at[0, theirs], recv_sem=sems.at[1, mine],
            device_id=device, device_id_type=MESH,
        )
        copy.start()
        pending.append(copy)

    def arrive(dst, sems, theirs, device):
        pltpu.make_async_remote_copy(
            src_ref=dst.at[theirs], dst_ref=dst.at[theirs], send_sem=sems.at[0, theirs], recv_sem=sems.at[1, theirs],
            device_id=device, device_id_type=MESH,
        ).wait_recv()

    def lanes_of(p):
        return pl.ds(pl.multiple_of(p * LANES, LANES), LANES)

    share_copy = pltpu.make_async_copy(share_ref.at[:, lanes_of(ai)], share_v, copy_sem)
    share_copy.start()

    barrier = pltpu.get_barrier_semaphore()

    @pl.loop(1, n)
    def _(d):
        t = (me + d) % n
        pl.semaphore_signal(barrier, inc=1, device_id=(t // grp, t % grp), device_id_type=MESH)

    pl.semaphore_wait(barrier, n - 1)

    for d in range(1, rb):
        p, device = type_peer(d)
        send(loy_ref.at[:, lanes_of(p)], loy, loy_s, ai, p, device)
    for d in range(1, rb):
        p, device = type_peer(d)
        send(info_ref, info, info_s, ai, p, device)
        send(mean0_ref, means.at[0], mean_s.at[0], ai, p, device)
    for d in range(1, rb):
        p, device = type_peer(d)
        send(wide_ref.at[:, lanes_of(p)], wide, wide_s, ai, p, device)

    wide[ai] = wide_ref[:, lanes_of(ai)]
    info[ai] = info_ref[...]
    loy[ai] = loy_ref[:, lanes_of(ai)]
    means[0, ai] = mean0_ref[...]

    for i in range(firms // LANES):
        order_col[i * LANES:(i + 1) * LANES, :] = columns(order_ref[0:1, i * LANES:(i + 1) * LANES])

    for d in range(1, rb):
        p, device = type_peer(d)
        arrive(loy, loy_s, p, device)
    for p in range(rb):
        tq[p * owned:(p + 1) * owned, :] = loy[p]
    for d in range(1, groups):
        q, device = market_peer(d)
        send(tq, tbl, tq_s, q_me, q, device)
    tbl[q_me] = tq[...]

    share_copy.wait()
    first = pl.multiple_of(q_me * qr, 8)
    mine_col = order_col[pl.ds(first, qr), :]
    number = lax.broadcasted_iota(jnp.int32, (qr, LANES), 1).astype(jnp.float32)
    my_share = jnp.zeros((qr, LANES), jnp.float32)
    for i in range(firms // LANES):
        pick = (mine_col == number + float(i * LANES)).astype(jnp.float32)
        my_share += jnp.dot(
            pick, share_v[i * LANES:(i + 1) * LANES, :],
            precision=lax.Precision.HIGHEST, preferred_element_type=jnp.float32,
        )
    my_share = jnp.log(my_share)

    for d in range(1, rb):
        p, device = type_peer(d)
        arrive(info, info_s, p, device)
        arrive(means.at[0], mean_s.at[0], p, device)
    for d in range(1, rb):
        p, device = type_peer(d)
        arrive(wide, wide_s, p, device)

    tm_own[...] = jnp.zeros_like(tm_own)

    @pl.loop(0, rb)
    def _(p):
        tm_own[...] += jnp.sum(wide[p, n_m * K:, :], axis=0, keepdims=True)

    for d in range(1, groups):
        q, device = market_peer(d)
        send(tm_own, tmass, tm_s, q_me, q, device)
    tmass[q_me] = tm_own[...]

    @pl.loop(0, rb)
    def _(p):
        row = lax.broadcasted_iota(jnp.int32, (n_m * K, rows), 0)
        lane = lax.broadcasted_iota(jnp.int32, (n_m * K, rows), 1)
        traits = jnp.zeros((n_m * K, rows), jnp.float32)
        for k in range(K):
            traits = jnp.where(row - (row // K) * K == k, info[p, k:k + 1, :], traits)
        traits = jnp.where(row // K == lane // J, traits, 0.0)
        taste[p] = lax.dot_general(
            traits, wide[p, :n_m * K, :], (((0,), (0,)), ((), ())),
            precision=lax.Precision.HIGHEST, preferred_element_type=jnp.float32,
        )
        for i in range(tiles):
            firm_row = info[p, K:K + 1, i * LANES:(i + 1) * LANES]
            firm_col = columns(firm_row)
            for f in range(firms // LANES):
                one_hot[p, i * LANES:(i + 1) * LANES, f * LANES:(f + 1) * LANES] = (
                    firm_col == order_ref[0:1, f * LANES:(f + 1) * LANES]
                ).astype(jnp.float32).astype(jnp.bfloat16)
            one_hot_t[p, :, i * LANES:(i + 1) * LANES] = (
                order_col[...] == firm_row
            ).astype(jnp.float32).astype(jnp.bfloat16)

    for d in range(1, groups):
        q, device = market_peer(d)
        arrive(tbl, tq_s, q, device)
        arrive(tmass, tm_s, q, device)
    log_mass = jnp.log(jnp.sum(tmass[...], axis=0))

    block = 2 * LANES
    per_block = block // J

    def contract(it):
        for q in range(groups):
            hi, lo = split_hi_lo(tbl[q])
            table_hl[q * qr:(q + 1) * qr, :LANES] = hi
            table_hl[q * qr:(q + 1) * qr, LANES:] = lo
        acc[...] = jnp.zeros_like(acc)

        @pl.loop(0, rb)
        def _(p):
            mean_rows = means[it, p]
            for h in range(rows // block):
                r0 = h * block
                both = jnp.dot(
                    one_hot[p, r0:r0 + block, :], table_hl[...], preferred_element_type=jnp.float32
                )
                mean_col = jnp.concatenate(
                    [columns(mean_rows[2 * h + i:2 * h + i + 1, :]) for i in range(2)], axis=0
                )
                expu = jnp.exp(both[:, :LANES] + both[:, LANES:] + mean_col + taste[p, r0:r0 + block, :])
                parts = []
                for m in range(per_block):
                    part = expu[m * J:(m + 1) * J, :]
                    mass = wide[p, n_m * K + h * per_block + m:n_m * K + h * per_block + m + 1, :]
                    parts.append(part * (mass / (1.0 + jnp.sum(part, axis=0, keepdims=True))))
                bought = jnp.concatenate(parts, axis=0)
                for i in range(2):
                    sums[it, p, 2 * h + i:2 * h + i + 1, :] = jnp.sum(
                        bought[i * LANES:(i + 1) * LANES, :].T, axis=0, keepdims=True
                    )
                hi, lo = split_hi_lo(bought)
                weighted[r0:r0 + block, :LANES] = hi
                weighted[r0:r0 + block, LANES:] = lo
            acc[...] += jnp.dot(one_hot_t[p], weighted[...], preferred_element_type=jnp.float32)

        for q in range(groups):
            totals[it, q] = acc[q * qr:(q + 1) * qr, :LANES] + acc[q * qr:(q + 1) * qr, LANES:]

    mean_now = mean0_ref[...]
    for it in range(ITERS):
        final = it == ITERS - 1
        if final:
            mine = tbl[q_me]
            for p in range(rb):
                old[p] = mine[p * owned:(p + 1) * owned, :]
            for d in range(1, rb):
                p, device = type_peer(d)
                send(old.at[p], old_in, old_s, ai, p, device)
            old_in[ai] = old[ai]
        contract(it)
        for d in range(1, groups):
            q, device = market_peer(d)
            send(totals.at[it, q], totals_in.at[it], totals_s.at[it], q_me, q, device)
        for d in range(1, rb):
            p, device = type_peer(d)
            send(sums.at[it, p], sums_in.at[it], sums_s.at[it], ai, p, device)
        sums_in[it, ai] = sums[it, ai]
        totals_in[it, q_me] = totals[it, q_me]

        for d in range(1, rb):
            p, device = type_peer(d)
            arrive(sums_in.at[it], sums_s.at[it], p, device)
        mean_now = mean_now + base_ref[...] - jnp.log(jnp.sum(sums_in[it], axis=0))
        if final:
            mean_out[...] = mean_now
        else:
            means[it + 1, ai] = mean_now
            for d in range(1, rb):
                p, device = type_peer(d)
                send(means.at[it + 1, ai], means.at[it + 1], mean_s.at[it + 1], ai, p, device)

        for d in range(1, groups):
            q, device = market_peer(d)
            arrive(totals_in.at[it], totals_s.at[it], q, device)
        gap_mine = my_share - (jnp.log(jnp.sum(totals_in[it], axis=0)) - log_mass)
        squares[it] = jnp.sum(gap_mine * gap_mine, axis=0, keepdims=True)

        @pl.loop(1, n)
        def _(d):
            t = (me + d) % n
            pltpu.make_async_remote_copy(
                src_ref=squares.at[it], dst_ref=squares_in.at[it, d - 1],
                send_sem=sq_s.at[0, it], recv_sem=sq_s.at[1, it],
                device_id=(t // grp, t % grp), device_id_type=MESH,
            ).start()

        if final:
            for p in range(rb):
                last[p] = gap_mine[p * owned:(p + 1) * owned, :]
            for d in range(1, rb):
                p, device = type_peer(d)
                send(last.at[p], last_in, last_s, ai, p, device)
            last_in[ai] = last[ai]
        else:
            gap[it, q_me] = gap_mine
            for d in range(1, groups):
                q, device = market_peer(d)
                send(gap.at[it, q_me], gap.at[it], gap_s.at[it], q_me, q, device)

        pltpu.make_async_copy(squares_in.at[it], squares_in.at[it], sq_s.at[1, it]).wait()
        total = jnp.sum(jnp.sum(squares_in[it], axis=0) + squares[it], axis=1, keepdims=True)
        clip = jnp.minimum(1.0, clip_target / jnp.sqrt(total / (firms * R) + norm_eps))

        if final:
            for d in range(1, rb):
                p, device = type_peer(d)
                arrive(old_in, old_s, p, device)
                arrive(last_in, last_s, p, device)
            for p in range(rb):
                loy_out[:, p * LANES:(p + 1) * LANES] = old_in[p] + clip * last_in[p]
        else:
            for d in range(1, groups):
                q, device = market_peer(d)
                arrive(gap.at[it], gap_s.at[it], q, device)
            for q in range(groups):
                tbl[q] = tbl[q] + clip * gap[it, q]
            for d in range(1, rb):
                p, device = type_peer(d)
                arrive(means.at[it + 1], mean_s.at[it + 1], p, device)

    for it in range(ITERS):
        pltpu.make_async_copy(squares_in.at[it], squares_in.at[it], sq_s.at[0, it]).wait()
    for copy in pending:
        copy.wait_send()


def local(
    mkt, grp,
    mean_utility, market_share, product_traits, taste_draws, taste_scale, type_weight,
    market_size, product_firm, firm_order, loyalty, firm_share,
):
    n_m, J, K = product_traits.shape
    firms, R = firm_share.shape
    owned = loyalty.shape[0]
    rb = R // LANES
    groups = mkt * grp // rb
    rows = n_m * J
    tiles = rows // LANES
    qr = firms // groups

    mass = market_size[:, None] * type_weight
    wide_own = jnp.concatenate([taste_draws.reshape(n_m * K, R), mass], axis=0)
    traits = (product_traits * taste_scale).reshape(rows, K).T
    firm = product_firm.astype(jnp.float32).reshape(1, rows)
    height = -(-(K + 1) // 8) * 8
    info_own = jnp.concatenate([traits, firm, jnp.zeros((height - K - 1, rows), jnp.float32)], axis=0)
    base = jnp.log(market_share) + jnp.log(jnp.sum(mass, axis=1))[:, None]
    order = firm_order.astype(jnp.float32).reshape(mkt // rb, rb, grp, owned)
    order = order.transpose(0, 2, 1, 3).reshape(1, firms)

    f32, bf16 = jnp.float32, jnp.bfloat16
    dma = pltpu.SemaphoreType.DMA
    vmem = pltpu.VMEM
    spec = pl.BlockSpec(memory_space=pltpu.VMEM)
    dims = (mkt, grp, rb, groups, n_m, J, K, firms, owned, R)
    scratch = [
        vmem((rb,) + wide_own.shape[:1] + (LANES,), f32),
        vmem((rb, height, rows), f32),
        vmem((rb, owned, LANES), f32),
        vmem((ITERS, rb, tiles, LANES), f32),
        vmem((groups, qr, LANES), f32),
        vmem((qr, LANES), f32),
        vmem((groups, 1, LANES), f32),
        vmem((1, LANES), f32),
        vmem((rb, rows, firms), bf16),
        vmem((rb, firms, rows), bf16),
        vmem((rb, rows, LANES), f32),
        vmem((firms, LANES), f32),
        vmem((firms, LANES), f32),
        vmem((rows, 2 * LANES), bf16),
        vmem((firms, 2 * LANES), bf16),
        vmem((firms, 2 * LANES), f32),
        vmem((ITERS, rb, tiles, LANES), f32),
        vmem((ITERS, rb, tiles, LANES), f32),
        vmem((ITERS, groups, qr, LANES), f32),
        vmem((ITERS, groups, qr, LANES), f32),
        vmem((ITERS - 1, groups, qr, LANES), f32),
        vmem((ITERS, 1, LANES), f32),
        vmem((ITERS, mkt * grp - 1, 1, LANES), f32),
        vmem((rb, owned, LANES), f32),
        vmem((rb, owned, LANES), f32),
        vmem((rb, owned, LANES), f32),
        vmem((rb, owned, LANES), f32),
        dma,
        dma((2, rb)), dma((2, rb)), dma((2, rb)),
        dma((ITERS, 2, rb)),
        dma((2, groups)), dma((2, groups)),
        dma((ITERS, 2, rb)),
        dma((ITERS, 2, groups)),
        dma((ITERS - 1, 2, groups)),
        dma((2, rb)), dma((2, rb)),
        dma((2, ITERS)),
    ]
    mean_new, loyalty_new = pl.pallas_call(
        functools.partial(kernel, dims),
        out_shape=(
            jax.ShapeDtypeStruct((tiles, LANES), f32),
            jax.ShapeDtypeStruct((owned, R), f32),
        ),
        in_specs=[spec] * 6 + [pl.BlockSpec(memory_space=pl.ANY)],
        out_specs=(spec, spec),
        scratch_shapes=scratch,
        compiler_params=pltpu.CompilerParams(
            collective_id=0, has_side_effects=True, vmem_limit_bytes=60 * 1024 * 1024
        ),
    )(
        wide_own, info_own, loyalty, base.reshape(tiles, LANES),
        mean_utility.reshape(tiles, LANES), order, firm_share,
    )
    return mean_new.reshape(n_m, J), loyalty_new


def solution(mesh):
    both = ("mkt", "grp")
    placed = (
        P(both, None), P(both, None), P(both, None, None), P(both, None, None), P(),
        P(both, None), P(both), P(both, None), P(), P(both, None), P(),
    )
    return jax.shard_map(
        functools.partial(local, mesh.shape["mkt"], mesh.shape["grp"]),
        mesh=mesh,
        in_specs=placed,
        out_specs=(P(both, None), P(both, None)),
        check_vma=False,
    )
```

```python
import functools
import math

import jax
import jax.numpy as jnp
from jax import lax
from jax.experimental import pallas as pl
from jax.experimental.pallas import tpu as pltpu
from jax.sharding import PartitionSpec as P

ITERS = 3
LANES = 128
MESH = pl.DeviceIdType.MESH

clip_target = 0.5
norm_eps = 1e-06


def columns(row):
    return jnp.broadcast_to(row, (LANES, LANES)).T


def split_hi_lo(x):
    hi = x.astype(jnp.bfloat16)
    lo = (x - hi.astype(jnp.float32)).astype(jnp.bfloat16)
    return hi, lo


def kernel(
    dims,
    size_ref, scale_ref, draws_ref, weight_ref, traits_ref, firm_ref, mean_ref, share_own_ref,
    loy_ref, order_ref, share_ref,
    mean_out, loy_out,
    draws, mass, info, loy, means, tbl, tq, tmass, tm_own,
    mass_own, info_own, lmat, one_hot, one_hot_t, taste, col, order_col, order_row, share_v, weighted, table_hl, acc,
    sums, sums_in, totals, totals_in, gap, squares, squares_in, old, old_in, last, last_in,
    copy_sem, draws_s, mass_s, info_s, loy_s, mean_s, tq_s, tm_s, sums_s, totals_s, gap_s, old_s, last_s, sq_s,
):
    mkt, grp, rb, groups, n_m, J, K, firms, owned, R = dims
    n = mkt * grp
    rows = n_m * J
    tiles = rows // LANES
    pair = LANES // J
    qr = firms // groups
    half = groups // 2
    a = lax.axis_index("mkt")
    b = lax.axis_index("grp")
    ao, ai = a // rb, a % rb
    q_me = ao * grp + b
    me = a * grp + b
    side = q_me // half

    barrier = pltpu.get_barrier_semaphore()

    @pl.loop(1, n)
    def _(d):
        t = (me + d) % n
        pl.semaphore_signal(barrier, inc=1, device_id=(t // grp, t % grp), device_id_type=MESH)

    def type_peer(d):
        p = (ai + d) % rb
        return p, (ao * rb + p, b)

    def market_device(q):
        return ((q // grp) * rb + ai, q % grp)

    def market_peer(d):
        q = (q_me + d) % groups
        return q, market_device(q)

    pending = []

    def send(src, dst, sems, mine, theirs, device):
        copy = pltpu.make_async_remote_copy(
            src_ref=src, dst_ref=dst.at[mine], send_sem=sems.at[0, theirs], recv_sem=sems.at[1, mine],
            device_id=device, device_id_type=MESH,
        )
        copy.start()
        pending.append(copy)

    def arrive(dst, sems, theirs, device):
        pltpu.make_async_remote_copy(
            src_ref=dst.at[theirs], dst_ref=dst.at[theirs], send_sem=sems.at[0, theirs], recv_sem=sems.at[1, theirs],
            device_id=device, device_id_type=MESH,
        ).wait_recv()

    def lanes_of(p):
        return pl.ds(pl.multiple_of(p * LANES, LANES), LANES)

    def pack(x):
        return jnp.concatenate([x[i * tiles:(i + 1) * tiles, :] for i in range(pair)], axis=1)

    share_copy = pltpu.make_async_copy(share_ref.at[:, lanes_of(ai)], share_v, copy_sem)
    share_copy.start()

    for k in range(K):
        info_own[k] = pack(traits_ref[k] * scale_ref[k])
    info_own[K] = pack(firm_ref[...].astype(jnp.float32))
    info_own[K + 1] = pack(mean_ref[...])
    for m in range(n_m):
        mass_own[m:m + 1, :] = weight_ref[m:m + 1, :] * size_ref[m]
    info[ai] = info_own[...]

    pl.semaphore_wait(barrier, n - 1)

    for d in range(1, rb):
        p, device = type_peer(d)
        send(loy_ref.at[:, lanes_of(p)], loy, loy_s, ai, p, device)
    for d in range(1, rb):
        p, device = type_peer(d)
        send(info_own, info, info_s, ai, p, device)
        send(draws_ref.at[:, lanes_of(p)], draws, draws_s, ai, p, device)
        send(mass_own.at[:, lanes_of(p)], mass, mass_s, ai, p, device)

    draws[ai] = draws_ref[:, lanes_of(ai)]
    mass[ai] = mass_own[:, lanes_of(ai)]
    loy[ai] = loy_ref[:, lanes_of(ai)]

    for i in range(firms // LANES):
        col[i * LANES:(i + 1) * LANES, :] = columns(order_ref[i:i + 1, :].astype(jnp.float32))
    for q in range(groups):
        for p in range(rb):
            src = (((q // grp) * rb + p) * grp + q % grp) * owned
            dst = (q * rb + p) * owned
            order_col[dst:dst + owned, :] = col[src:src + owned, :]
    for i in range(firms // LANES):
        order_row[0:1, i * LANES:(i + 1) * LANES] = order_col[i * LANES:(i + 1) * LANES, :].T[0:1, :]

    for d in range(1, rb):
        p, device = type_peer(d)
        arrive(loy, loy_s, p, device)
    for p in range(rb):
        tq[p * owned:(p + 1) * owned, :] = loy[p]
    for d in range(1, groups):
        q, device = market_peer(d)
        send(tq, tbl, tq_s, q_me, q, device)
    tbl[q_me] = tq[...]

    row = lax.broadcasted_iota(jnp.int32, (n_m * K, LANES), 0)
    lane = lax.broadcasted_iota(jnp.int32, (n_m * K, LANES), 1)
    trait_of = row // n_m
    offset = row % n_m - (lane // J) * tiles

    def prepare(p):
        for i in range(tiles):
            traits = jnp.zeros((n_m * K, LANES), jnp.float32)
            for k in range(K):
                traits = jnp.where(trait_of == k, info[p, k, i:i + 1, :], traits)
            lmat[:, i * LANES:(i + 1) * LANES] = jnp.where(offset == i, traits, 0.0)
        taste[p] = lax.dot_general(
            lmat[...], draws[p], (((0,), (0,)), ((), ())),
            precision=lax.Precision.HIGHEST, preferred_element_type=jnp.float32,
        )
        for i in range(tiles):
            firm_row = info[p, K, i:i + 1, :]
            firm_col = columns(firm_row)
            for f in range(firms // LANES):
                one_hot[p, i * LANES:(i + 1) * LANES, f * LANES:(f + 1) * LANES] = (
                    firm_col == order_row[0:1, f * LANES:(f + 1) * LANES]
                ).astype(jnp.float32).astype(jnp.bfloat16)
            one_hot_t[p, :, i * LANES:(i + 1) * LANES] = (
                order_col[...] == firm_row
            ).astype(jnp.float32).astype(jnp.bfloat16)

    prepare(ai)

    share_copy.wait()
    first = pl.multiple_of(q_me * qr, 8)
    mine_col = order_col[pl.ds(first, qr), :]
    number = lax.broadcasted_iota(jnp.int32, (qr, LANES), 1).astype(jnp.float32)
    my_share = jnp.zeros((qr, LANES), jnp.float32)
    for i in range(firms // LANES):
        pick = (mine_col == number + float(i * LANES)).astype(jnp.float32)
        my_share += jnp.dot(
            pick, share_v[i * LANES:(i + 1) * LANES, :],
            precision=lax.Precision.HIGHEST, preferred_element_type=jnp.float32,
        )
    my_share = jnp.log(my_share)

    share_own = share_own_ref[...]
    base = jnp.log(share_own) + jnp.log(jnp.sum(mass_own[...], axis=1, keepdims=True))
    base = pack(base)

    for d in range(1, groups):
        q, device = market_peer(d)
        arrive(tbl, tq_s, q, device)

    def split_table():
        for q in range(groups):
            hi, lo = split_hi_lo(tbl[q])
            table_hl[q * qr:(q + 1) * qr, :LANES] = hi
            table_hl[q * qr:(q + 1) * qr, LANES:] = lo

    per_block = 2
    block = per_block * LANES

    def shares(it, p):
        mean_rows = info[p, K + 1] if it == 0 else means[it - 1, p]
        for h in range(rows // block):
            r0 = h * block
            both = jnp.dot(
                one_hot[p, r0:r0 + block, :], table_hl[...], preferred_element_type=jnp.float32
            )
            mean_col = jnp.concatenate(
                [columns(mean_rows[i:i + 1, :]) for i in range(h * per_block, (h + 1) * per_block)], axis=0
            )
            expu = jnp.exp(both[:, :LANES] + both[:, LANES:] + mean_col + taste[p, r0:r0 + block, :])
            parts = []
            for i in range(per_block):
                for s in range(pair):
                    part = expu[i * LANES + s * J:i * LANES + (s + 1) * J, :]
                    m = s * tiles + h * per_block + i
                    parts.append(
                        part * (mass[p, m:m + 1, :] / (1.0 + jnp.sum(part, axis=0, keepdims=True)))
                    )
            bought = jnp.concatenate(parts, axis=0)
            for i in range(per_block):
                at = h * per_block + i
                sums[it, p, at:at + 1, :] = jnp.sum(
                    bought[i * LANES:(i + 1) * LANES, :].T, axis=0, keepdims=True
                )
            hi, lo = split_hi_lo(bought)
            weighted[p, r0:r0 + block, :LANES] = hi
            weighted[p, r0:r0 + block, LANES:] = lo

    def half_totals(it, which):
        begin = pl.multiple_of(which * (half * qr), 16)
        acc[...] = jnp.zeros_like(acc)

        @pl.loop(0, rb)
        def _(p):
            acc[...] += jnp.dot(
                one_hot_t[p, pl.ds(begin, half * qr), :], weighted[p], preferred_element_type=jnp.float32
            )

        for j in range(half):
            totals[it, which * half + j] = (
                acc[j * qr:(j + 1) * qr, :LANES] + acc[j * qr:(j + 1) * qr, LANES:]
            )

    mean_now = pack(mean_ref[...])
    log_mass = None
    for it in range(ITERS):
        final = it == ITERS - 1
        if final:
            mine = tbl[q_me]
            for p in range(rb):
                old[p] = mine[p * owned:(p + 1) * owned, :]
            for d in range(1, rb):
                p, device = type_peer(d)
                send(old.at[p], old_in, old_s, ai, p, device)
            old_in[ai] = old[ai]
        split_table()
        if it == 0:
            shares(0, ai)

            @pl.loop(1, rb)
            def _(d):
                p, device = type_peer(d)
                arrive(info, info_s, p, device)
                arrive(draws, draws_s, p, device)
                arrive(mass, mass_s, p, device)
                prepare(p)
                shares(0, p)

            tm_own[...] = jnp.zeros_like(tm_own)
            for p in range(rb):
                tm_own[...] += jnp.sum(mass[p], axis=0, keepdims=True)
            for d in range(1, groups):
                q, device = market_peer(d)
                send(tm_own, tmass, tm_s, q_me, q, device)
            tmass[q_me] = tm_own[...]
        else:
            @pl.loop(0, rb)
            def _(p):
                shares(it, p)

        for d in range(1, rb):
            p, device = type_peer(d)
            send(sums.at[it, p], sums_in.at[it], sums_s.at[it], ai, p, device)
        sums_in[it, ai] = sums[it, ai]

        half_totals(it, 1 - side)
        for j in range(half):
            q = (1 - side) * half + (q_me + j) % half
            send(totals.at[it, q], totals_in.at[it], totals_s.at[it], q_me, q, market_device(q))
        half_totals(it, side)
        for j in range(1, half):
            q = side * half + (q_me + j) % half
            send(totals.at[it, q], totals_in.at[it], totals_s.at[it], q_me, q, market_device(q))
        totals_in[it, q_me] = totals[it, q_me]

        for d in range(1, rb):
            p, device = type_peer(d)
            arrive(sums_in.at[it], sums_s.at[it], p, device)
        mean_now = mean_now + base - jnp.log(jnp.sum(sums_in[it], axis=0))
        if final:
            for i in range(pair):
                mean_out[i * tiles:(i + 1) * tiles, :] = mean_now[:, i * J:(i + 1) * J]
        else:
            means[it, ai] = mean_now
            for d in range(1, rb):
                p, device = type_peer(d)
                send(means.at[it, ai], means.at[it], mean_s.at[it], ai, p, device)

        if it == 0:
            for d in range(1, groups):
                q, device = market_peer(d)
                arrive(tmass, tm_s, q, device)
            log_mass = jnp.log(jnp.sum(tmass[...], axis=0))
        for d in range(1, groups):
            q, device = market_peer(d)
            arrive(totals_in.at[it], totals_s.at[it], q, device)
        gap_mine = my_share - (jnp.log(jnp.sum(totals_in[it], axis=0)) - log_mass)
        squares[it] = jnp.sum(gap_mine * gap_mine, axis=0, keepdims=True)

        @pl.loop(1, n)
        def _(d):
            t = (me + d) % n
            pltpu.make_async_remote_copy(
                src_ref=squares.at[it], dst_ref=squares_in.at[it, d - 1],
                send_sem=sq_s.at[0, it], recv_sem=sq_s.at[1, it],
                device_id=(t // grp, t % grp), device_id_type=MESH,
            ).start()

        if final:
            for p in range(rb):
                last[p] = gap_mine[p * owned:(p + 1) * owned, :]
            for d in range(1, rb):
                p, device = type_peer(d)
                send(last.at[p], last_in, last_s, ai, p, device)
            last_in[ai] = last[ai]
        else:
            gap[it, q_me] = gap_mine
            for d in range(1, groups):
                q, device = market_peer(d)
                send(gap.at[it, q_me], gap.at[it], gap_s.at[it], q_me, q, device)

        pltpu.make_async_copy(squares_in.at[it], squares_in.at[it], sq_s.at[1, it]).wait()
        total = jnp.sum(jnp.sum(squares_in[it], axis=0) + squares[it], axis=1, keepdims=True)
        clip = jnp.minimum(1.0, clip_target / jnp.sqrt(total / (firms * R) + norm_eps))

        if final:
            for d in range(1, rb):
                p, device = type_peer(d)
                arrive(old_in, old_s, p, device)
                arrive(last_in, last_s, p, device)
            for p in range(rb):
                loy_out[:, p * LANES:(p + 1) * LANES] = old_in[p] + clip * last_in[p]
        else:
            for d in range(1, groups):
                q, device = market_peer(d)
                arrive(gap.at[it], gap_s.at[it], q, device)
            for q in range(groups):
                tbl[q] = tbl[q] + clip * gap[it, q]
            for d in range(1, rb):
                p, device = type_peer(d)
                arrive(means.at[it], mean_s.at[it], p, device)

    for it in range(ITERS):
        pltpu.make_async_copy(squares_in.at[it], squares_in.at[it], sq_s.at[0, it]).wait()
    for copy in pending:
        copy.wait_send()


def local(
    mkt, grp,
    mean_utility, market_share, product_traits, taste_draws, taste_scale, type_weight,
    market_size, product_firm, firm_order, loyalty, firm_share,
):
    n_m, J, K = product_traits.shape
    firms, R = firm_share.shape
    owned = loyalty.shape[0]
    rb = R // LANES
    groups = mkt * grp // rb
    rows = n_m * J
    tiles = rows // LANES
    qr = firms // groups

    f32, bf16 = jnp.float32, jnp.bfloat16
    dma = pltpu.SemaphoreType.DMA
    vmem = pltpu.VMEM
    spec = pl.BlockSpec(memory_space=pltpu.VMEM)
    smem = pl.BlockSpec(memory_space=pltpu.SMEM)
    dims = (mkt, grp, rb, groups, n_m, J, K, firms, owned, R)
    scratch = [
        vmem((rb, n_m * K, LANES), f32),
        vmem((rb, n_m, LANES), f32),
        vmem((rb, K + 2, tiles, LANES), f32),
        vmem((rb, owned, LANES), f32),
        vmem((ITERS - 1, rb, tiles, LANES), f32),
        vmem((groups, qr, LANES), f32),
        vmem((qr, LANES), f32),
        vmem((groups, 1, LANES), f32),
        vmem((1, LANES), f32),
        vmem((n_m, R), f32),
        vmem((K + 2, tiles, LANES), f32),
        vmem((n_m * K, rows), f32),
        vmem((rb, rows, firms), bf16),
        vmem((rb, firms, rows), bf16),
        vmem((rb, rows, LANES), f32),
        vmem((firms, LANES), f32),
        vmem((firms, LANES), f32),
        vmem((1, firms), f32),
        vmem((firms, LANES), f32),
        vmem((rb, rows, 2 * LANES), bf16),
        vmem((firms, 2 * LANES), bf16),
        vmem((firms // 2, 2 * LANES), f32),
        vmem((ITERS, rb, tiles, LANES), f32),
        vmem((ITERS, rb, tiles, LANES), f32),
        vmem((ITERS, groups, qr, LANES), f32),
        vmem((ITERS, groups, qr, LANES), f32),
        vmem((ITERS - 1, groups, qr, LANES), f32),
        vmem((ITERS, 1, LANES), f32),
        vmem((ITERS, mkt * grp - 1, 1, LANES), f32),
        vmem((rb, owned, LANES), f32),
        vmem((rb, owned, LANES), f32),
        vmem((rb, owned, LANES), f32),
        vmem((rb, owned, LANES), f32),
        dma,
        dma((2, rb)), dma((2, rb)), dma((2, rb)), dma((2, rb)),
        dma((ITERS - 1, 2, rb)),
        dma((2, groups)), dma((2, groups)),
        dma((ITERS, 2, rb)),
        dma((ITERS, 2, groups)),
        dma((ITERS - 1, 2, groups)),
        dma((2, rb)), dma((2, rb)),
        dma((2, ITERS)),
    ]
    return pl.pallas_call(
        functools.partial(kernel, dims),
        out_shape=(
            jax.ShapeDtypeStruct((n_m, J), f32),
            jax.ShapeDtypeStruct((owned, R), f32),
        ),
        in_specs=[smem] * 2 + [spec] * 8 + [pl.BlockSpec(memory_space=pl.ANY)],
        out_specs=(spec, spec),
        scratch_shapes=scratch,
        compiler_params=pltpu.CompilerParams(
            collective_id=0, has_side_effects=True, vmem_limit_bytes=60 * 1024 * 1024
        ),
    )(
        market_size, taste_scale, taste_draws.transpose(1, 0, 2).reshape(n_m * K, R), type_weight,
        product_traits.transpose(2, 0, 1), product_firm, mean_utility, market_share,
        loyalty, firm_order.reshape(firms // LANES, LANES), firm_share,
    )


def solution(mesh):
    both = ("mkt", "grp")
    placed = (
        P(both, None), P(both, None), P(both, None, None), P(both, None, None), P(),
        P(both, None), P(both), P(both, None), P(), P(both, None), P(),
    )
    return jax.shard_map(
        functools.partial(local, mesh.shape["mkt"], mesh.shape["grp"]),
        mesh=mesh,
        in_specs=placed,
        out_specs=(P(both, None), P(both, None)),
        check_vma=False,
    )
```
